32 devices in a mesh: band: 16 (over z, x, core), ga: 2 (over y).
Axes of the slice: x: 2, y: 2, z: 4, core: 2. Of those that a mesh axis runs over, the one named last changes fastest.
Arguments:
- psi: float32 [2, 4096, 65536], P(None, 'band', 'ga'), may hold values from -0.0234375 to 0.0234375
- hx: float32 [2, 256, 65536], P(None, 'band', 'ga'), may hold values from -6 to 6
Outputs:
- h_sub: float32 [2, 4096, 256], P(None, ('band', 'ga'))
The draws below stay inside these ranges and needn't reach their ends.
All inputs are finite; a program needn't handle non-finite values.
Results may differ from the reference program's by a relative error of at most 0.00007.
Values sent between devices are 32-bit elements; how exact they have to be, the bound alone decides.
A program may use at most 192 MiB of HBM per device.

```python
import jax
import jax.numpy as jnp
from jax import lax

NB = 4096
NG = 65536
NBLK = 256


def level_of(stream_key, dims, shards, smallest, high):
    def one(position, shards_of):
        draws = jax.random.uniform(jax.random.fold_in(jax.random.fold_in(stream_key, 6), position), (shards_of,), jnp.float32, smallest / len(shards), high / len(shards))
        return jnp.repeat(jnp.exp(draws), dims[position] // shards_of).reshape((-1,) + (1,) * (len(dims) - position - 1))

    gain = one(*shards[0])
    for cut in shards[1:]:
        gain = gain * one(*cut)
    return gain


def gaussian(key, extent, scale, reach, split=(), held_as=jnp.bfloat16):
    factor_of = level_of(key, extent, split, -0.22, 0.18) if split else 1.0
    entries = jax.random.normal(key, extent, jnp.float32) * scale * factor_of
    return jnp.minimum(jnp.maximum(entries, -reach), reach).astype(held_as)


def setup_inputs(seed: int = 0) -> dict:
    key_list = jax.random.split(jax.random.key(seed), 3)
    psi = gaussian(key_list[0], (2, NB, NG), NG ** -0.5, 0.0234375, ((1, 16), (2, 2)), jnp.float32)
    hx = gaussian(key_list[1], (2, NBLK, NG), 1.0, 6.0, ((1, 16), (2, 2)), jnp.float32)
    return dict(psi=psi, hx=hx)


def contract(left, right):
    return lax.dot_general(left, right, (((1,), (1,)), ((), ())), precision=lax.Precision.HIGHEST, preferred_element_type=jnp.float32)


def reference(psi, hx):
    real_part = contract(psi[0], hx[0]) + contract(psi[1], hx[1])
    imag_part = contract(psi[0], hx[1]) - contract(psi[1], hx[0])
    return jnp.stack([real_part, imag_part], axis=0)
```

```python
import jax
import jax.numpy as jnp
from jax import lax
from jax.sharding import PartitionSpec as P

SHARES = (22, 10)


def contract(left, right):
    return lax.dot_general(
        left,
        right,
        (((1,), (1,)), ((), ())),
        precision=lax.Precision.HIGH,
        preferred_element_type=jnp.float32,
    )


def per_device(psi, hx):
    parts, rows, depth = psi.shape
    unit = depth // sum(SHARES)
    bands = psi.reshape(parts * rows, depth)
    total = None
    first = 0
    pieces = []
    for share in SHARES:
        last = first + share * unit
        piece = lax.all_gather(hx[:, :, first:last], "band", axis=1, tiled=True)
        pieces.append((first, last, piece))
        first = last
    for first, last, piece in pieces:
        product = contract(bands[:, first:last], piece.reshape(-1, last - first))
        total = product if total is None else total + product
    vectors = total.shape[1] // parts
    real_left, imag_left = total[:rows], total[rows:]
    real_tile = real_left[:, :vectors] + imag_left[:, vectors:]
    imag_tile = real_left[:, vectors:] - imag_left[:, :vectors]
    partial_value = jnp.stack([real_tile, imag_tile], axis=0)
    n = lax.axis_size("ga")
    me = lax.axis_index("ga")
    height = rows // n

    def block(owner):
        return lax.dynamic_slice_in_dim(partial_value, owner * height, height, axis=1)

    result = block(me)
    for step in range(1, n):
        ring = [(i, (i + step) % n) for i in range(n)]
        result = result + lax.ppermute(block(lax.rem(me + step, n)), "ga", ring)
    return result


def solution(mesh):
    in_specs = (P(None, "band", "ga"), P(None, "band", "ga"))
    out_specs = P(None, ("band", "ga"), None)
    return jax.shard_map(
        per_device, mesh=mesh, in_specs=in_specs, out_specs=out_specs, check_vma=False
    )
```
